128 devices in a mesh: mem: 4 (over z), lat: 32 (over y, x, core).
Axes of the slice: x: 4, y: 4, z: 4, core: 2. Of those that a mesh axis runs over, the one named last changes fastest.
Arguments:
- ensemble: bfloat16 [32, 72, 32, 1440], P('mem', None, 'lat'), may hold values from -6 to 6
- truth: bfloat16 [72, 32, 1440], P(None, 'lat'), may hold values from -6 to 6
- row_weight: float32 [32], P('lat'), may hold values from 0.3 to 7, as said below
Outputs:
- loss: float32 [], replicated
- gradient: bfloat16 [32, 72, 32, 1440], P('mem', None, 'lat')
The draws below stay inside these ranges and needn't reach their ends.
Inputs may be any that keep to these rules, and one draw needn't show every extreme that they name: `row_weight`: positive.
All inputs are finite; a program needn't handle non-finite values.
Results may differ from the reference program's by a relative error of at most 0.003.
Values may be sent and summed in bfloat16 or wider, within the bound.
A program may use at most 128 MiB of HBM per device.

```python
import jax
import jax.numpy as jnp
from jax import lax

C = 72
LON = 1440
M = 32
NLAT = 32


def draw_row_weight(key, part):
    rows = jnp.arange(NLAT).astype(jnp.float32)
    rising = 1.0 + 3.0 * rows / NLAT
    noise = jnp.exp(jax.random.uniform(key, (NLAT,), jnp.float32, jnp.log(0.6), jnp.log(1.6)))
    return (rising * noise).astype(jnp.float32)


def level_of(key, extent, pieces, least, high):
    def one(axis_at, blocks):
        heights = jax.random.uniform(jax.random.fold_in(jax.random.fold_in(key, 6), axis_at), (blocks,), jnp.float32, least / len(pieces), high / len(pieces))
        return jnp.repeat(jnp.exp(heights), extent[axis_at] // blocks).reshape((-1,) + (1,) * (len(extent) - axis_at - 1))

    gain = one(*pieces[0])
    for cut in pieces[1:]:
        gain = gain * one(*cut)
    return gain


def centred(rng, shape, scale, most, shards=(), held_as=jnp.bfloat16):
    array = jax.random.normal(rng, shape, jnp.float32) * scale
    if len(shards) > 0:
        array = level_of(rng, shape, shards, -0.22, 0.18) * array
    return jnp.clip(array, min=-most, max=most).astype(held_as)


def setup_inputs(seed: int = 0) -> dict:
    key_list = jax.random.split(jax.random.key(seed), 4)
    return {
        "ensemble": centred(key_list[0], (M, C, NLAT, LON), 1.0, 6.0, ((0, 4), (2, 32))),
        "truth": centred(key_list[1], (C, NLAT, LON), 1.0, 6.0, ((1, 32),)),
        "row_weight": draw_row_weight(jax.random.fold_in(key_list[3], 71), 0),
    }


def reference(ensemble, truth, row_weight):
    members = ensemble.shape[0]
    channels = ensemble.shape[1]
    by_channel = jnp.moveaxis(ensemble, 1, 0)
    weight = row_weight.astype(jnp.float32)[:, None]

    def channel(pair):
        values = pair[0].astype(jnp.float32)
        target = pair[1].astype(jnp.float32)

        def visit(index, carry):
            spread, count = carry
            other = lax.dynamic_index_in_dim(values, index, 0, keepdims=False)
            diff = values - other
            return spread + jnp.abs(diff), count + jnp.sign(diff)

        zeros = jnp.zeros(values.shape, jnp.float32)
        spread, count = lax.fori_loop(0, members, visit, (zeros, zeros))
        skill = values - target
        cell = jnp.sum(jnp.abs(skill), axis=0) / members - jnp.sum(spread, axis=0) / (2.0 * members * (members - 1))
        partial_value = jnp.sum(weight * cell)
        grad = (weight[None] * (jnp.sign(skill) - count / (members - 1))).astype(jnp.bfloat16)
        return partial_value, grad

    partials, grads = lax.map(channel, (by_channel, truth))
    loss = jnp.sum(partials) / (channels * ensemble.shape[2] * ensemble.shape[3])
    return loss, jnp.moveaxis(grads, 0, 1)
```

```python
import functools

import jax
import jax.numpy as jnp
from jax import lax
from jax.experimental import pallas as pl
from jax.experimental.pallas import tpu as pltpu
from jax.sharding import PartitionSpec as P

MESH = pl.DeviceIdType.MESH
GROUPS = 4
SUB = 8
LANE = 128
CHUNKS = ((0, 512), (512, 512), (1024, 384))
FULL = 1408
EXTRA = 16
SHARE = EXTRA // GROUPS


def sign_of(left, right):
    return jnp.where(left > right, 1.0, jnp.where(left < right, -1.0, 0.0))


def counts_of(x):
    members = x.shape[0]
    count = jnp.zeros_like(x)
    for step in range(1, members // 2 + 1):
        if 2 * step == members:
            s = sign_of(x[:step], x[step:])
            count = count + jnp.concatenate([s, -s], axis=0)
        else:
            s = sign_of(x, jnp.concatenate([x[step:], x[:step]], axis=0))
            count = count + (s - jnp.concatenate([s[-step:], s[:-step]], axis=0))
    return count


def tile_terms(x, t, weight, pairs):
    count = counts_of(x) * (1.0 / pairs)
    skill = jnp.abs(x - t[None])
    cell = jnp.sum(skill - x * count, axis=0)
    grad = weight * (sign_of(x, t[None]) - count)
    return cell, grad.astype(jnp.bfloat16)


def kernel(
    lat_dims, scale, ens, tru, w_ref, out, loss, xin, tin, ex, tex, rv, rex, gv, gex, oex,
    part, stage, load_sem, send_v, recv_v, send_g, recv_g, send_s, recv_s,
):
    me = lax.axis_index("mem")
    lat = lax.axis_index("lat")
    ny, nx, nc = lat_dims
    core = lax.rem(lat, nc)
    x_at = lax.rem(lat // nc, nx)
    y_at = lat // (nc * nx)
    local = ens.shape[0]
    members = local * GROUPS
    rows = ens.shape[1]

    def peer(axis, d):
        if axis == "mem":
            return {"mem": lax.rem(me + d, GROUPS)}
        if axis == "core":
            return {"lat": (y_at * nx + x_at) * nc + lax.rem(core + d, nc)}
        if axis == "x":
            return {"lat": (y_at * nx + lax.rem(x_at + d, nx)) * nc + core}
        return {"lat": (lax.rem(y_at + d, ny) * nx + x_at) * nc + core}

    axes = [("core", nc, core), ("x", nx, x_at), ("y", ny, y_at), ("mem", GROUPS, me)]
    axes = [a for a in axes if a[1] > 1]

    barrier = pltpu.get_barrier_semaphore()
    count = 0
    for axis, size, _ in axes:
        for d in range(1, size):
            pl.semaphore_signal(barrier, inc=1, device_id=peer(axis, d), device_id_type=MESH)
            count += 1
    load_x = pltpu.make_async_copy(ens, xin, load_sem.at[0])
    load_t = pltpu.make_async_copy(tru, tin, load_sem.at[1])
    load_x.start()
    load_t.start()
    load_x.wait()
    load_t.wait()
    pl.semaphore_wait(barrier, count)

    def values_copy(c, d):
        to = lax.rem(me + d, GROUPS)
        if c == len(CHUNKS):
            src, dst = ex.at[:, pl.ds(SHARE * to, SHARE)], rex.at[d - 1]
        else:
            at, wide = CHUNKS[c]
            src = xin.at[:, pl.ds(2 * to, 2), :, pl.ds(at, wide)]
            dst = rv.at[d - 1, :, :, :, pl.ds(at, wide)]
        return pltpu.make_async_remote_copy(
            src_ref=src, dst_ref=dst, send_sem=send_v.at[c, d - 1], recv_sem=recv_v.at[c, d - 1],
            device_id=peer("mem", d), device_id_type=MESH,
        )

    def grads_copy(c, d):
        if c == len(CHUNKS):
            src, dst = gex.at[d - 1], oex.at[:, pl.ds(SHARE * me, SHARE)]
        else:
            at, wide = CHUNKS[c]
            src = gv.at[d - 1, :, :, :, pl.ds(at, wide)]
            dst = out.at[:, pl.ds(2 * me, 2), :, pl.ds(at, wide)]
        return pltpu.make_async_remote_copy(
            src_ref=src, dst_ref=dst, send_sem=send_g.at[c, d - 1], recv_sem=recv_g.at[c, d - 1],
            device_id=peer("mem", GROUPS - d), device_id_type=MESH,
        )

    order = (0, len(CHUNKS)) + tuple(range(1, len(CHUNKS)))
    hops = (2, 1, 3)
    for d in hops:
        values_copy(0, d).start()

    def pack(src, dst):
        for k in range(FULL // LANE):
            dst[k] = src[rows - 1, :, k * LANE : (k + 1) * LANE]
        wide = src.shape[-1] - FULL
        per = LANE // wide
        for g in range(EXTRA - FULL // LANE):
            parts = [
                src[r, :, FULL:].astype(jnp.float32)
                if r < rows
                else jnp.zeros((SUB, wide), jnp.float32)
                for r in range(g * per, (g + 1) * per)
            ]
            dst[FULL // LANE + g] = jnp.concatenate(parts, axis=1).astype(jnp.bfloat16)

    pack(tin, tex)

    @pl.loop(0, local)
    def _(m):
        pack(xin.at[m], ex.at[m])

    for c in order[1:]:
        for d in hops:
            values_copy(c, d).start()

    weight = w_ref[0]
    part[...] = jnp.zeros_like(part)

    def chunk_tiles(c):
        if c == len(CHUNKS):

            def body(k, carry):
                mine = ex[:, SHARE * me + k]
                x = jnp.concatenate([mine] + [rex[d, :, k] for d in range(GROUPS - 1)], axis=0)
                cell, grad = tile_terms(
                    x.astype(jnp.float32), tex[SHARE * me + k].astype(jnp.float32), weight, members - 1
                )
                part[...] += cell
                oex[:, SHARE * me + k] = grad[:local]
                for d in range(GROUPS - 1):
                    gex[d, :, k] = grad[(d + 1) * local : (d + 2) * local]
                return carry

            lax.fori_loop(0, SHARE, body, 0)
        else:
            at, wide = CHUNKS[c]
            tiles = wide // LANE

            def body(k, carry):
                r = k // tiles
                lanes = pl.ds(pl.multiple_of(at + (k - r * tiles) * LANE, LANE), LANE)
                mine = xin[:, 2 * me + r, :, lanes]
                x = jnp.concatenate(
                    [mine] + [rv[d, :, r, :, lanes] for d in range(GROUPS - 1)], axis=0
                )
                cell, grad = tile_terms(
                    x.astype(jnp.float32),
                    tin[2 * me + r, :, lanes].astype(jnp.float32),
                    weight,
                    members - 1,
                )
                part[...] += cell
                out[:, 2 * me + r, :, lanes] = grad[:local]
                for d in range(GROUPS - 1):
                    gv[d, :, r, :, lanes] = grad[(d + 1) * local : (d + 2) * local]
                return carry

            lax.fori_loop(0, 2 * tiles, body, 0)

    for c in order:
        for d in hops:
            values_copy(c, d).wait_recv()
        chunk_tiles(c)
        for d in hops:
            grads_copy(c, d).start()

    part[...] = part[...] * (weight * scale)
    at = 0
    for number, (axis, size, mine) in enumerate(axes):
        copies = []
        for d in range(1, size):
            copies.append(
                pltpu.make_async_remote_copy(
                    src_ref=part.at[number] if False else part,
                    dst_ref=stage.at[number, mine],
                    send_sem=send_s.at[at],
                    recv_sem=recv_s.at[at],
                    device_id=peer(axis, d),
                    device_id_type=MESH,
                )
            )
            at += 1
        for copy in copies:
            copy.start()
        stage[number, mine] = part[...]
        for copy in copies:
            copy.wait()
        total = stage[number, 0]
        for k in range(1, size):
            total = total + stage[number, k]
        part[...] = total
    loss[0, 0] = jnp.sum(part[...])

    for d in hops:
        grads_copy(len(CHUNKS), d).wait_recv()

    @pl.loop(0, local)
    def _(m):
        for k in range(FULL // LANE):
            out[m, rows - 1, :, k * LANE : (k + 1) * LANE] = oex[m, k]
        wide = out.shape[-1] - FULL
        per = LANE // wide
        for g in range(-(-rows // per)):
            tile = oex[m, FULL // LANE + g].astype(jnp.float32)
            for j in range(per):
                if g * per + j < rows:
                    out[m, g * per + j, :, FULL:] = tile[:, j * wide : (j + 1) * wide].astype(
                        jnp.bfloat16
                    )

    for c in range(len(CHUNKS)):
        for d in hops:
            grads_copy(c, d).wait_recv()
    for c in order:
        for d in hops:
            values_copy(c, d).wait_send()
            grads_copy(c, d).wait_send()


def on_device(lat_dims, total_cells, ensemble, truth, row_weight):
    local, channels, _, lon = ensemble.shape
    rows = channels // SUB
    peers = GROUPS - 1
    n_copies = len(CHUNKS) + 1
    bf = jnp.bfloat16
    n_stage = sum(s - 1 for s in lat_dims) + peers
    loss, out = pl.pallas_call(
        functools.partial(
            lambda l, s, e, t, w, o, z, *rest: kernel(l, s, e, t, w, z, o, *rest),
            lat_dims,
            1.0 / (local * GROUPS) / total_cells,
        ),
        out_shape=(
            jax.ShapeDtypeStruct((1, 1), jnp.float32),
            jax.ShapeDtypeStruct((local, rows, SUB, lon), bf),
        ),
        in_specs=[
            pl.BlockSpec(memory_space=pl.ANY),
            pl.BlockSpec(memory_space=pl.ANY),
            pl.BlockSpec(memory_space=pltpu.SMEM),
        ],
        out_specs=(
            pl.BlockSpec(memory_space=pltpu.SMEM),
            pl.BlockSpec(memory_space=pltpu.VMEM),
        ),
        scratch_shapes=[
            pltpu.VMEM((local, rows, SUB, lon), bf),
            pltpu.VMEM((rows, SUB, lon), bf),
            pltpu.VMEM((local, EXTRA, SUB, LANE), bf),
            pltpu.VMEM((EXTRA, SUB, LANE), bf),
            pltpu.VMEM((peers, local, 2, SUB, FULL), bf),
            pltpu.VMEM((peers, local, SHARE, SUB, LANE), bf),
            pltpu.VMEM((peers, local, 2, SUB, FULL), bf),
            pltpu.VMEM((peers, local, SHARE, SUB, LANE), bf),
            pltpu.VMEM((local, EXTRA, SUB, LANE), bf),
            pltpu.VMEM((SUB, LANE), jnp.float32),
            pltpu.VMEM((4, 4, SUB, LANE), jnp.float32),
            pltpu.SemaphoreType.DMA((2,)),
            pltpu.SemaphoreType.DMA((n_copies, peers)),
            pltpu.SemaphoreType.DMA((n_copies, peers)),
            pltpu.SemaphoreType.DMA((n_copies, peers)),
            pltpu.SemaphoreType.DMA((n_copies, peers)),
            pltpu.SemaphoreType.DMA((n_stage,)),
            pltpu.SemaphoreType.DMA((n_stage,)),
        ],
        compiler_params=pltpu.CompilerParams(
            collective_id=0, has_side_effects=True, vmem_limit_bytes=48 * 1024 * 1024
        ),
        name="crps_exchange",
    )(
        ensemble.reshape(local, rows, SUB, lon),
        truth.reshape(rows, SUB, lon),
        row_weight,
    )
    return loss.reshape(()), out.reshape(ensemble.shape)


def solution(mesh, lat_dims=(4, 4, 2)):
    def whole(ensemble, truth, row_weight):
        cells = truth.size
        step = jax.shard_map(
            functools.partial(on_device, lat_dims, cells),
            mesh=mesh,
            in_specs=(P("mem", None, "lat", None), P(None, "lat", None), P("lat")),
            out_specs=(P(), P("mem", None, "lat", None)),
            check_vma=False,
        )
        return step(ensemble, truth, row_weight)

    return whole
```

```python
import functools

import jax
import jax.numpy as jnp
from jax import lax
from jax.experimental import pallas as pl
from jax.experimental.pallas import tpu as pltpu
from jax.sharding import PartitionSpec as P

MESH = pl.DeviceIdType.MESH
GROUPS = 4
SUB = 8
LANE = 128
CHUNKS = ((0, 512), (512, 384), (896, 384), (1280, 128))
FULL = 1408
DEAL = (3, 4, 3, 4)
EXTRA = sum(DEAL)
FIRST = tuple(sum(DEAL[:rank]) for rank in range(GROUPS))


def sign_of(left, right):
    return jnp.where(left > right, 1.0, jnp.where(left < right, -1.0, 0.0))


def counts_of(x):
    members = x.shape[0]
    count = jnp.zeros_like(x)
    for step in range(1, members // 2 + 1):
        if 2 * step == members:
            s = sign_of(x[:step], x[step:])
            count = count + jnp.concatenate([s, -s], axis=0)
        else:
            s = sign_of(x, jnp.concatenate([x[step:], x[:step]], axis=0))
            count = count + (s - jnp.concatenate([s[-step:], s[:-step]], axis=0))
    return count


def tile_terms(x, t, weight, pairs):
    count = counts_of(x) * (1.0 / pairs)
    skill = jnp.abs(x - t[None])
    cell = jnp.sum(skill - x * count, axis=0)
    grad = weight * (sign_of(x, t[None]) - count)
    return cell, grad.astype(jnp.bfloat16)


def kernel(
    plane, scale, ens, tru, w_hbm, out, loss, xin, tin, ex, tex, rv, rex, gv, gex, oex,
    cells, part, gift, stage, totals, w_ref, load_sem, send_v, recv_v, send_g, recv_g, send_s, recv_s,
    send_t, recv_t, ready,
):
    me = lax.axis_index("mem")
    lat = lax.axis_index("lat")
    local = ens.shape[0]
    members = local * GROUPS
    rows = ens.shape[1]

    def column(d):
        return {"mem": lax.rem(me + d, GROUPS)}

    even = lax.rem(me, 2) == 0
    odd = lax.rem(me, 2) == 1

    barrier = pltpu.get_barrier_semaphore()

    def greet(where):
        pl.semaphore_signal(barrier, inc=1, device_id=where, device_id_type=MESH)

    @pl.when(odd)
    def _():
        greet(column(2))

    @pl.when(even)
    def _():
        for d in (1, 3):
            greet(column(d))

        @pl.loop(1, plane)
        def _(k):
            greet({"lat": lax.rem(lat + k, plane)})

    load_x = pltpu.make_async_copy(ens, xin, load_sem.at[0])
    load_t = pltpu.make_async_copy(tru, tin, load_sem.at[1])
    load_w = pltpu.make_async_copy(w_hbm, w_ref, load_sem.at[2])
    load_w.start()
    load_x.start()
    load_t.start()

    @pl.when(odd)
    def _():
        pl.semaphore_wait(barrier, GROUPS - 1)
        for d in (1, 3):
            pl.semaphore_signal(ready, inc=1, device_id=column(d), device_id_type=MESH)

    @pl.when(even)
    def _():
        pl.semaphore_wait(ready, 2)


    n = len(CHUNKS)

    def remote(src, dst, send, recv, d):
        return pltpu.make_async_remote_copy(
            src_ref=src, dst_ref=dst, send_sem=send, recv_sem=recv,
            device_id=column(d), device_id_type=MESH,
        )

    def values_copy(c, d, owner=None):
        to = lax.rem(me + d, GROUPS)
        if c == n:
            src = ex.at[:, pl.ds(FIRST[owner], DEAL[owner])]
            dst = rex.at[d - 1, :, pl.ds(0, DEAL[owner])]
        else:
            at, wide = CHUNKS[c]
            src = ens.at[:, pl.ds(2 * to, 2), :, pl.ds(at, wide)]
            dst = rv.at[d - 1, :, :, :, pl.ds(at, wide)]
        return remote(src, dst, send_v.at[c, d - 1], recv_v.at[c, d - 1], d)

    def grads_copy(c, d, owner=None):
        if c == n:
            src = gex.at[d - 1, :, pl.ds(0, DEAL[owner])]
            dst = oex.at[:, pl.ds(FIRST[owner], DEAL[owner])]
        else:
            at, wide = CHUNKS[c]
            src = gv.at[d - 1, :, :, :, pl.ds(at, wide)]
            dst = out.at[:, pl.ds(2 * me, 2), :, pl.ds(at, wide)]
        return remote(src, dst, send_g.at[c, d - 1], recv_g.at[c, d - 1], GROUPS - d)

    def one(make, c, d, act, owner):
        if c < n:
            act(make(c, d))
            return
        for rank in range(GROUPS):

            @pl.when(owner == rank)
            def _():
                act(make(c, d, rank))

    def each(make, c, act, to_peer):
        for d in hops:
            one(make, c, d, act, lax.rem(me + d, GROUPS) if to_peer else me)

    order = (0, n) + tuple(range(1, n))

    def send_back(pieces):
        for c, d in pieces:
            one(grads_copy, c, d, lambda copy: copy.start(), me)

    hops = (2, 1, 3)
    start = lambda copy: copy.start()
    landed = lambda copy: copy.wait_recv()
    left = lambda copy: copy.wait_send()
    each(values_copy, 0, start, True)
    load_x.wait()
    load_t.wait()
    load_w.wait()

    def pack(src, dst):
        for k in range(FULL // LANE):
            dst[k] = src[rows - 1, :, k * LANE : (k + 1) * LANE]
        wide = src.shape[-1] - FULL
        per = LANE // wide
        for g in range(EXTRA - FULL // LANE):
            parts = [
                src[r, :, FULL:].astype(jnp.float32)
                if r < rows
                else jnp.zeros((SUB, wide), jnp.float32)
                for r in range(g * per, (g + 1) * per)
            ]
            dst[FULL // LANE + g] = jnp.concatenate(parts, axis=1).astype(jnp.bfloat16)

    pack(tin, tex)

    @pl.loop(0, local)
    def _(m):
        pack(xin.at[m], ex.at[m])

    for c in order[1:-2]:
        each(values_copy, c, start, True)

    def send_values(pieces):
        for c, d in pieces:
            values_copy(c, d).start()

    @pl.when(even)
    def _():
        send_values([(c, d) for c in order[-2:] for d in (1, 3)] + [(c, 2) for c in order[-2:]])

    @pl.when(odd)
    def _():
        send_values([(c, 2) for c in order[-2:]] + [(c, d) for c in order[-2:] for d in (1, 3)])


    weight = w_ref[0]
    cells[...] = jnp.zeros_like(cells)

    def chunk_tiles(c):
        if c == n:
            first, many = FIRST[0], DEAL[0]
            for rank in range(1, GROUPS):
                first = jnp.where(me == rank, FIRST[rank], first)
                many = jnp.where(me == rank, DEAL[rank], many)

            def body(k, carry):
                mine = ex[:, first + k]
                x = jnp.concatenate([mine] + [rex[d, :, k] for d in range(GROUPS - 1)], axis=0)
                cell, grad = tile_terms(
                    x.astype(jnp.float32), tex[first + k].astype(jnp.float32), weight, members - 1
                )
                cells[...] += cell
                oex[:, first + k] = grad[:local]
                for d in range(GROUPS - 1):
                    gex[d, :, k] = grad[(d + 1) * local : (d + 2) * local]
                return carry

            lax.fori_loop(0, many, body, 0)
        else:
            at, wide = CHUNKS[c]
            tiles = wide // LANE

            def body(k, carry):
                r = k // tiles
                lanes = pl.ds(pl.multiple_of(at + (k - r * tiles) * LANE, LANE), LANE)
                mine = xin[:, 2 * me + r, :, lanes]
                x = jnp.concatenate(
                    [mine] + [rv[d, :, r, :, lanes] for d in range(GROUPS - 1)], axis=0
                )
                cell, grad = tile_terms(
                    x.astype(jnp.float32),
                    tin[2 * me + r, :, lanes].astype(jnp.float32),
                    weight,
                    members - 1,
                )
                cells[...] += cell
                out[:, 2 * me + r, :, lanes] = grad[:local]
                for d in range(GROUPS - 1):
                    gv[d, :, r, :, lanes] = grad[(d + 1) * local : (d + 2) * local]
                return carry

            lax.fori_loop(0, 2 * tiles, body, 0)

    for c in order:
        each(values_copy, c, landed, False)
        chunk_tiles(c)

        @pl.when(even)
        def _():
            if c != order[-1]:
                send_back([(c, d) for d in (2, 1, 3)])

        @pl.when(odd)
        def _():
            send_back([(c, d) for d in ((3, 1, 2) if c == 0 else (1, 2))])

    part[...] = jnp.sum(cells[...], axis=0, keepdims=True) * (weight * scale)
    hand = pltpu.make_async_remote_copy(
        src_ref=part, dst_ref=gift, send_sem=send_t.at[0], recv_sem=recv_t.at[0],
        device_id=column(1), device_id_type=MESH,
    )

    def tell(half, d):
        return pltpu.make_async_remote_copy(
            src_ref=part, dst_ref=totals.at[half], send_sem=send_t.at[d],
            recv_sem=recv_t.at[1 + half], device_id=column(d), device_id_type=MESH,
        )

    half = me // 2

    @pl.when(odd)
    def _():
        hand.start()
        send_back([(c, 3) for c in order[1:]])

    @pl.when(even)
    def _():
        pl.semaphore_wait(barrier, plane - 1)
        hand.wait_recv()
        part[...] += gift[...]

        def share(k):
            return pltpu.make_async_remote_copy(
                src_ref=part, dst_ref=stage.at[lat], send_sem=send_s.at[k - 1],
                recv_sem=recv_s.at[k - 1], device_id={"lat": lax.rem(lat + k, plane)},
                device_id_type=MESH,
            )

        @pl.loop(1, plane)
        def _(k):
            share(k).start()

        stage[lat] = part[...]

        @pl.loop(1, plane)
        def _(k):
            share(k).wait()

        part[...] = jnp.sum(stage[...], axis=0)
        for d in hops:
            tell(half, d).start()
        totals[half] = part[...]
        send_back([(order[-1], d) for d in hops])

    each(grads_copy, n, landed, True)

    @pl.loop(0, local)
    def _(m):
        for k in range(FULL // LANE):
            out[m, rows - 1, :, k * LANE : (k + 1) * LANE] = oex[m, k]
        wide = out.shape[-1] - FULL
        per = LANE // wide
        for g in range(-(-rows // per)):
            tile = oex[m, FULL // LANE + g].astype(jnp.float32)
            for j in range(per):
                if g * per + j < rows:
                    out[m, g * per + j, :, FULL:] = tile[:, j * wide : (j + 1) * wide].astype(
                        jnp.bfloat16
                    )

    @pl.when(even)
    def _():
        tell(1 - half, 2).wait_recv()
        for d in hops:
            tell(half, d).wait_send()

    @pl.when(odd)
    def _():
        for k in range(2):
            tell(k, 1).wait_recv()
        hand.wait_send()

    loss[...] = jnp.full(loss.shape, jnp.sum(totals[0] + totals[1]))

    for c in range(n):
        each(grads_copy, c, landed, True)
    for c in order:
        each(values_copy, c, left, True)
        each(grads_copy, c, left, False)


def hand_over(loss, grads, loss_out, grads_out, loss_at, sems):
    copies = [
        pltpu.make_async_copy(grads.at[m], grads_out.at[m], sems.at[m])
        for m in range(grads.shape[0])
    ]
    for copy in copies:
        copy.start()
    loss_at[0] = loss[0, 0]
    last = pltpu.make_async_copy(loss_at, loss_out, sems.at[grads.shape[0]])
    last.start()
    for copy in copies:
        copy.wait()
    last.wait()


def on_device(total_cells, ensemble, truth, row_weight):
    local, channels, _, lon = ensemble.shape
    rows = channels // SUB
    peers = GROUPS - 1
    plane = lax.axis_size("lat")
    n_copies = len(CHUNKS) + 1
    bf = jnp.bfloat16
    loss, out = pl.pallas_call(
        functools.partial(
            lambda l, s, e, t, w, o, z, *rest: kernel(l, s, e, t, w, z, o, *rest),
            plane,
            1.0 / (local * GROUPS) / total_cells,
        ),
        out_shape=(
            jax.ShapeDtypeStruct((1, LANE), jnp.float32),
            jax.ShapeDtypeStruct((local, rows, SUB, lon), bf),
        ),
        in_specs=[
            pl.BlockSpec(memory_space=pl.ANY),
            pl.BlockSpec(memory_space=pl.ANY),
            pl.BlockSpec(memory_space=pltpu.HBM),
        ],
        out_specs=(
            pl.BlockSpec(memory_space=pltpu.VMEM),
            pl.BlockSpec(memory_space=pltpu.VMEM),
        ),
        scratch_shapes=[
            pltpu.VMEM((local, rows, SUB, lon), bf),
            pltpu.VMEM((rows, SUB, lon), bf),
            pltpu.VMEM((local, EXTRA, SUB, LANE), bf),
            pltpu.VMEM((EXTRA, SUB, LANE), bf),
            pltpu.VMEM((peers, local, 2, SUB, FULL), bf),
            pltpu.VMEM((peers, local, max(DEAL), SUB, LANE), bf),
            pltpu.VMEM((peers, local, 2, SUB, FULL), bf),
            pltpu.VMEM((peers, local, max(DEAL), SUB, LANE), bf),
            pltpu.VMEM((local, EXTRA, SUB, LANE), bf),
            pltpu.VMEM((SUB, LANE), jnp.float32),
            pltpu.VMEM((1, LANE), jnp.float32),
            pltpu.VMEM((1, LANE), jnp.float32),
            pltpu.VMEM((plane, 1, LANE), jnp.float32),
            pltpu.VMEM((2, 1, LANE), jnp.float32),
            pltpu.SMEM((1,), jnp.float32),
            pltpu.SemaphoreType.DMA((3,)),
            pltpu.SemaphoreType.DMA((n_copies, peers)),
            pltpu.SemaphoreType.DMA((n_copies, peers)),
            pltpu.SemaphoreType.DMA((n_copies, peers)),
            pltpu.SemaphoreType.DMA((n_copies, peers)),
            pltpu.SemaphoreType.DMA((plane - 1,)),
            pltpu.SemaphoreType.DMA((plane - 1,)),
            pltpu.SemaphoreType.DMA((GROUPS,)),
            pltpu.SemaphoreType.DMA((3,)),
            pltpu.SemaphoreType.REGULAR,
        ],
        compiler_params=pltpu.CompilerParams(
            collective_id=0, has_side_effects=True, vmem_limit_bytes=48 * 1024 * 1024
        ),
        name="crps_exchange",
    )(
        pltpu.with_memory_space_constraint(ensemble.reshape(local, rows, SUB, lon), pltpu.HBM),
        pltpu.with_memory_space_constraint(truth.reshape(rows, SUB, lon), pltpu.HBM),
        row_weight,
    )
    loss, out = pl.pallas_call(
        hand_over,
        out_shape=(
            jax.ShapeDtypeStruct((1,), jnp.float32),
            jax.ShapeDtypeStruct(out.shape, out.dtype),
        ),
        in_specs=[pl.BlockSpec(memory_space=pltpu.VMEM)] * 2,
        out_specs=(pl.BlockSpec(memory_space=pl.ANY), pl.BlockSpec(memory_space=pl.ANY)),
        scratch_shapes=[pltpu.SMEM((1,), jnp.float32), pltpu.SemaphoreType.DMA((local + 1,))],
        compiler_params=pltpu.CompilerParams(vmem_limit_bytes=4 * 1024 * 1024),
        name="hand_over",
    )(loss, out)
    return loss.reshape(()), out.reshape(ensemble.shape)


def solution(mesh):
    def whole(ensemble, truth, row_weight):
        cells = truth.size
        step = jax.shard_map(
            functools.partial(on_device, cells),
            mesh=mesh,
            in_specs=(P("mem", None, "lat", None), P(None, "lat", None), P("lat")),
            out_specs=(P(), P("mem", None, "lat", None)),
            check_vma=False,
        )
        return step(ensemble, truth, row_weight)

    return whole
```

```python
import functools

import jax
import jax.numpy as jnp
from jax import lax
from jax.experimental import pallas as pl
from jax.experimental.pallas import tpu as pltpu
from jax.sharding import PartitionSpec as P

MESH = pl.DeviceIdType.MESH
GROUPS = 4
SUB = 8
LANE = 128
CHUNKS = ((0, 512), (512, 384), (896, 384), (1280, 128))
FULL = 1408
DEAL = (3, 4, 3, 4)
EXTRA = sum(DEAL)
FIRST = tuple(sum(DEAL[:rank]) for rank in range(GROUPS))


def sign_of(left, right):
    return jnp.where(left > right, 1.0, jnp.where(left < right, -1.0, 0.0))


def counts_of(x):
    members = x.shape[0]
    count = jnp.zeros_like(x)
    for step in range(1, members // 2 + 1):
        if 2 * step == members:
            s = sign_of(x[:step], x[step:])
            count = count + jnp.concatenate([s, -s], axis=0)
        else:
            s = sign_of(x, jnp.concatenate([x[step:], x[:step]], axis=0))
            count = count + (s - jnp.concatenate([s[-step:], s[:-step]], axis=0))
    return count


def tile_terms(x, t, weight, pairs):
    count = counts_of(x) * (1.0 / pairs)
    skill = jnp.abs(x - t[None])
    cell = jnp.sum(skill - x * count, axis=0)
    grad = weight * (sign_of(x, t[None]) - count)
    return cell, grad.astype(jnp.bfloat16)


def kernel(
    plane, scale, ens, tru, w_hbm, out, loss, xin, tin, ex, tex, rv, rex, gv, gex, oex,
    cells, part, gift, stage, totals, w_ref, load_sem, send_v, recv_v, send_g, recv_g, send_s, recv_s,
    send_t, recv_t, ready,
):
    me = lax.axis_index("mem")
    lat = lax.axis_index("lat")
    local = ens.shape[0]
    members = local * GROUPS
    rows = ens.shape[1]

    def column(d):
        return {"mem": lax.rem(me + d, GROUPS)}

    even = lax.rem(me, 2) == 0
    odd = lax.rem(me, 2) == 1

    barrier = pltpu.get_barrier_semaphore()

    def greet(where):
        pl.semaphore_signal(barrier, inc=1, device_id=where, device_id_type=MESH)

    @pl.when(odd)
    def _():
        greet(column(2))

    @pl.when(even)
    def _():
        for d in (1, 3):
            greet(column(d))

        @pl.loop(1, plane)
        def _(k):
            greet({"lat": lax.rem(lat + k, plane)})

    load_x = pltpu.make_async_copy(ens, xin, load_sem.at[0])
    load_t = pltpu.make_async_copy(tru, tin, load_sem.at[1])
    load_w = pltpu.make_async_copy(w_hbm, w_ref, load_sem.at[2])
    load_w.start()
    load_x.start()
    load_t.start()

    @pl.when(odd)
    def _():
        pl.semaphore_wait(barrier, GROUPS - 1)
        pl.semaphore_signal(ready, inc=1, device_id=column(3), device_id_type=MESH)

    @pl.when(even)
    def _():
        pl.semaphore_wait(ready, 1)


    n = len(CHUNKS)

    def remote(src, dst, send, recv, d):
        return pltpu.make_async_remote_copy(
            src_ref=src, dst_ref=dst, send_sem=send, recv_sem=recv,
            device_id=column(d), device_id_type=MESH,
        )

    def values_copy(c, d, owner=None):
        to = lax.rem(me + d, GROUPS)
        if c == n:
            src = ex.at[:, pl.ds(FIRST[owner], DEAL[owner])]
            dst = rex.at[d - 1, :, pl.ds(0, DEAL[owner])]
        else:
            at, wide = CHUNKS[c]
            src = xin.at[:, pl.ds(2 * to, 2), :, pl.ds(at, wide)]
            dst = rv.at[d - 1, :, :, :, pl.ds(at, wide)]
        return remote(src, dst, send_v.at[c, d - 1], recv_v.at[c, d - 1], d)

    def grads_copy(c, d, owner=None):
        if c == n:
            src = gex.at[d - 1, :, pl.ds(0, DEAL[owner])]
            dst = oex.at[:, pl.ds(FIRST[owner], DEAL[owner])]
        else:
            at, wide = CHUNKS[c]
            src = gv.at[d - 1, :, :, :, pl.ds(at, wide)]
            dst = out.at[:, pl.ds(2 * me, 2), :, pl.ds(at, wide)]
        return remote(src, dst, send_g.at[c, d - 1], recv_g.at[c, d - 1], GROUPS - d)

    def one(make, c, d, act, owner):
        if c < n:
            act(make(c, d))
            return
        for rank in range(GROUPS):

            @pl.when(owner == rank)
            def _():
                act(make(c, d, rank))

    def each(make, c, act, to_peer):
        for d in hops:
            one(make, c, d, act, lax.rem(me + d, GROUPS) if to_peer else me)

    order = (0, n) + tuple(range(1, n))

    def send_back(pieces):
        for c, d in pieces:
            one(grads_copy, c, d, lambda copy: copy.start(), me)

    hops = (2, 1, 3)
    start = lambda copy: copy.start()
    landed = lambda copy: copy.wait_recv()
    left = lambda copy: copy.wait_send()
    load_x.wait()
    each(values_copy, 0, start, True)
    load_t.wait()
    load_w.wait()

    def pack(src, dst):
        for k in range(FULL // LANE):
            dst[k] = src[rows - 1, :, k * LANE : (k + 1) * LANE]
        wide = src.shape[-1] - FULL
        per = LANE // wide
        for g in range(EXTRA - FULL // LANE):
            parts = [
                src[r, :, FULL:].astype(jnp.float32)
                if r < rows
                else jnp.zeros((SUB, wide), jnp.float32)
                for r in range(g * per, (g + 1) * per)
            ]
            dst[FULL // LANE + g] = jnp.concatenate(parts, axis=1).astype(jnp.bfloat16)

    pack(tin, tex)

    @pl.loop(0, local)
    def _(m):
        pack(xin.at[m], ex.at[m])

    for c in order[1:]:
        each(values_copy, c, start, True)

    weight = w_ref[0]
    cells[...] = jnp.zeros_like(cells)

    def chunk_tiles(c):
        if c == n:
            first, many = FIRST[0], DEAL[0]
            for rank in range(1, GROUPS):
                first = jnp.where(me == rank, FIRST[rank], first)
                many = jnp.where(me == rank, DEAL[rank], many)

            def body(k, carry):
                mine = ex[:, first + k]
                x = jnp.concatenate([mine] + [rex[d, :, k] for d in range(GROUPS - 1)], axis=0)
                cell, grad = tile_terms(
                    x.astype(jnp.float32), tex[first + k].astype(jnp.float32), weight, members - 1
                )
                cells[...] += cell
                oex[:, first + k] = grad[:local]
                for d in range(GROUPS - 1):
                    gex[d, :, k] = grad[(d + 1) * local : (d + 2) * local]
                return carry

            lax.fori_loop(0, many, body, 0)
        else:
            at, wide = CHUNKS[c]
            tiles = wide // LANE

            def body(k, carry):
                r = k // tiles
                lanes = pl.ds(pl.multiple_of(at + (k - r * tiles) * LANE, LANE), LANE)
                mine = xin[:, 2 * me + r, :, lanes]
                x = jnp.concatenate(
                    [mine] + [rv[d, :, r, :, lanes] for d in range(GROUPS - 1)], axis=0
                )
                cell, grad = tile_terms(
                    x.astype(jnp.float32),
                    tin[2 * me + r, :, lanes].astype(jnp.float32),
                    weight,
                    members - 1,
                )
                cells[...] += cell
                out[:, 2 * me + r, :, lanes] = grad[:local]
                for d in range(GROUPS - 1):
                    gv[d, :, r, :, lanes] = grad[(d + 1) * local : (d + 2) * local]
                return carry

            lax.fori_loop(0, 2 * tiles, body, 0)

    for c in order:
        each(values_copy, c, landed, False)
        chunk_tiles(c)

        @pl.when(even)
        def _():
            if c != order[-1]:
                send_back([(c, d) for d in (2, 1, 3)])

        @pl.when(odd)
        def _():
            send_back([(c, d) for d in ((3, 1, 2) if c == 0 else (1, 2))])

    part[...] = jnp.sum(cells[...], axis=0, keepdims=True) * (weight * scale)
    hand = pltpu.make_async_remote_copy(
        src_ref=part, dst_ref=gift, send_sem=send_t.at[0], recv_sem=recv_t.at[0],
        device_id=column(1), device_id_type=MESH,
    )

    def tell(half, d):
        return pltpu.make_async_remote_copy(
            src_ref=part, dst_ref=totals.at[half], send_sem=send_t.at[d],
            recv_sem=recv_t.at[1 + half], device_id=column(d), device_id_type=MESH,
        )

    half = me // 2

    @pl.when(odd)
    def _():
        hand.start()
        send_back([(c, 3) for c in order[1:]])

    @pl.when(even)
    def _():
        pl.semaphore_wait(barrier, plane - 1)
        hand.wait_recv()
        part[...] += gift[...]

        def share(k):
            return pltpu.make_async_remote_copy(
                src_ref=part, dst_ref=stage.at[lat], send_sem=send_s.at[k - 1],
                recv_sem=recv_s.at[k - 1], device_id={"lat": lax.rem(lat + k, plane)},
                device_id_type=MESH,
            )

        @pl.loop(1, plane)
        def _(k):
            share(k).start()

        stage[lat] = part[...]

        @pl.loop(1, plane)
        def _(k):
            share(k).wait()

        part[...] = jnp.sum(stage[...], axis=0)
        for d in hops:
            tell(half, d).start()
        totals[half] = part[...]
        send_back([(order[-1], d) for d in hops])

    each(grads_copy, n, landed, True)

    @pl.loop(0, local)
    def _(m):
        for k in range(FULL // LANE):
            out[m, rows - 1, :, k * LANE : (k + 1) * LANE] = oex[m, k]
        wide = out.shape[-1] - FULL
        per = LANE // wide
        for g in range(-(-rows // per)):
            tile = oex[m, FULL // LANE + g].astype(jnp.float32)
            for j in range(per):
                if g * per + j < rows:
                    out[m, g * per + j, :, FULL:] = tile[:, j * wide : (j + 1) * wide].astype(
                        jnp.bfloat16
                    )

    @pl.when(even)
    def _():
        tell(1 - half, 2).wait_recv()
        for d in hops:
            tell(half, d).wait_send()

    @pl.when(odd)
    def _():
        for k in range(2):
            tell(k, 1).wait_recv()
        hand.wait_send()

    loss[...] = jnp.full(loss.shape, jnp.sum(totals[0] + totals[1]))

    for c in range(n):
        each(grads_copy, c, landed, True)
    for c in order:
        each(values_copy, c, left, True)
        each(grads_copy, c, left, False)


def hand_over(loss, grads, loss_out, grads_out, loss_at, sems):
    copies = [
        pltpu.make_async_copy(grads.at[m], grads_out.at[m], sems.at[m])
        for m in range(grads.shape[0])
    ]
    for copy in copies:
        copy.start()
    loss_at[0] = loss[0, 0]
    last = pltpu.make_async_copy(loss_at, loss_out, sems.at[grads.shape[0]])
    last.start()
    for copy in copies:
        copy.wait()
    last.wait()


def on_device(total_cells, ensemble, truth, row_weight):
    local, channels, _, lon = ensemble.shape
    rows = channels // SUB
    peers = GROUPS - 1
    plane = lax.axis_size("lat")
    n_copies = len(CHUNKS) + 1
    bf = jnp.bfloat16
    loss, out = pl.pallas_call(
        functools.partial(
            lambda l, s, e, t, w, o, z, *rest: kernel(l, s, e, t, w, z, o, *rest),
            plane,
            1.0 / (local * GROUPS) / total_cells,
        ),
        out_shape=(
            jax.ShapeDtypeStruct((1, LANE), jnp.float32),
            jax.ShapeDtypeStruct((local, rows, SUB, lon), bf),
        ),
        in_specs=[
            pl.BlockSpec(memory_space=pl.ANY),
            pl.BlockSpec(memory_space=pl.ANY),
            pl.BlockSpec(memory_space=pltpu.HBM),
        ],
        out_specs=(
            pl.BlockSpec(memory_space=pltpu.VMEM),
            pl.BlockSpec(memory_space=pltpu.VMEM),
        ),
        scratch_shapes=[
            pltpu.VMEM((local, rows, SUB, lon), bf),
            pltpu.VMEM((rows, SUB, lon), bf),
            pltpu.VMEM((local, EXTRA, SUB, LANE), bf),
            pltpu.VMEM((EXTRA, SUB, LANE), bf),
            pltpu.VMEM((peers, local, 2, SUB, FULL), bf),
            pltpu.VMEM((peers, local, max(DEAL), SUB, LANE), bf),
            pltpu.VMEM((peers, local, 2, SUB, FULL), bf),
            pltpu.VMEM((peers, local, max(DEAL), SUB, LANE), bf),
            pltpu.VMEM((local, EXTRA, SUB, LANE), bf),
            pltpu.VMEM((SUB, LANE), jnp.float32),
            pltpu.VMEM((1, LANE), jnp.float32),
            pltpu.VMEM((1, LANE), jnp.float32),
            pltpu.VMEM((plane, 1, LANE), jnp.float32),
            pltpu.VMEM((2, 1, LANE), jnp.float32),
            pltpu.SMEM((1,), jnp.float32),
            pltpu.SemaphoreType.DMA((3,)),
            pltpu.SemaphoreType.DMA((n_copies, peers)),
            pltpu.SemaphoreType.DMA((n_copies, peers)),
            pltpu.SemaphoreType.DMA((n_copies, peers)),
            pltpu.SemaphoreType.DMA((n_copies, peers)),
            pltpu.SemaphoreType.DMA((plane - 1,)),
            pltpu.SemaphoreType.DMA((plane - 1,)),
            pltpu.SemaphoreType.DMA((GROUPS,)),
            pltpu.SemaphoreType.DMA((3,)),
            pltpu.SemaphoreType.REGULAR,
        ],
        compiler_params=pltpu.CompilerParams(
            collective_id=0, has_side_effects=True, vmem_limit_bytes=48 * 1024 * 1024
        ),
        name="crps_exchange",
    )(
        pltpu.with_memory_space_constraint(ensemble.reshape(local, rows, SUB, lon), pltpu.HBM),
        pltpu.with_memory_space_constraint(truth.reshape(rows, SUB, lon), pltpu.HBM),
        row_weight,
    )
    loss, out = pl.pallas_call(
        hand_over,
        out_shape=(
            jax.ShapeDtypeStruct((1,), jnp.float32),
            jax.ShapeDtypeStruct(out.shape, out.dtype),
        ),
        in_specs=[pl.BlockSpec(memory_space=pltpu.VMEM)] * 2,
        out_specs=(pl.BlockSpec(memory_space=pl.ANY), pl.BlockSpec(memory_space=pl.ANY)),
        scratch_shapes=[pltpu.SMEM((1,), jnp.float32), pltpu.SemaphoreType.DMA((local + 1,))],
        compiler_params=pltpu.CompilerParams(vmem_limit_bytes=4 * 1024 * 1024),
        name="hand_over",
    )(loss, out)
    return loss.reshape(()), out.reshape(ensemble.shape)


def solution(mesh):
    def whole(ensemble, truth, row_weight):
        cells = truth.size
        step = jax.shard_map(
            functools.partial(on_device, cells),
            mesh=mesh,
            in_specs=(P("mem", None, "lat", None), P(None, "lat", None), P("lat")),
            out_specs=(P(), P("mem", None, "lat", None)),
            check_vma=False,
        )
        return step(ensemble, truth, row_weight)

    return whole
```

```python
import functools

import jax
import jax.numpy as jnp
from jax import lax
from jax.experimental import pallas as pl
from jax.experimental.pallas import tpu as pltpu
from jax.sharding import PartitionSpec as P

MESH = pl.DeviceIdType.MESH
GROUPS = 4
SUB = 8
LANE = 128
CHUNKS = ((0, 512), (512, 384), (896, 384), (1280, 128))
FULL = 1408
DEAL = (3, 4, 3, 4)
EXTRA = sum(DEAL)
FIRST = tuple(sum(DEAL[:rank]) for rank in range(GROUPS))


def spread_out(x):
    tiny = jnp.minimum(jnp.maximum(x, -(2.0**-113)), 2.0**-113)
    return tiny * 2.0**66 * 2.0**67 + x * 2.0**124


def sign_of(left, right):
    return jnp.minimum(jnp.maximum(left - right, -1.0), 1.0)


def counts_of(x):
    members = x.shape[0]
    count = jnp.zeros_like(x)
    for step in range(1, members // 2 + 1):
        if 2 * step == members:
            s = sign_of(x[:step], x[step:])
            count = count + jnp.concatenate([s, -s], axis=0)
        else:
            s = sign_of(x, jnp.concatenate([x[step:], x[:step]], axis=0))
            count = count + (s - jnp.concatenate([s[-step:], s[:-step]], axis=0))
    return count


def tile_terms(x, t, weight, pairs):
    place = spread_out(x)
    count = counts_of(place) * (1.0 / pairs)
    skill = jnp.abs(x - t[None])
    cell = jnp.sum(skill - x * count, axis=0)
    grad = weight * (sign_of(place, spread_out(t)[None]) - count)
    return cell, grad.astype(jnp.bfloat16)


def kernel(
    plane, scale, ens, tru, w_hbm, out, loss, xin, tin, ex, tex, rv, rex, gv, gex, oex,
    cells, part, gift, stage, totals, w_ref, load_sem, send_v, recv_v, send_g, recv_g, send_s, recv_s,
    send_t, recv_t, ready,
):
    me = lax.axis_index("mem")
    lat = lax.axis_index("lat")
    local = ens.shape[0]
    members = local * GROUPS
    rows = ens.shape[1]

    def column(d):
        return {"mem": lax.rem(me + d, GROUPS)}

    even = lax.rem(me, 2) == 0
    odd = lax.rem(me, 2) == 1

    barrier = pltpu.get_barrier_semaphore()

    def greet(where):
        pl.semaphore_signal(barrier, inc=1, device_id=where, device_id_type=MESH)

    @pl.when(odd)
    def _():
        greet(column(2))

    @pl.when(even)
    def _():
        for d in (1, 3):
            greet(column(d))

        @pl.loop(1, plane)
        def _(k):
            greet({"lat": lax.rem(lat + k, plane)})

    load_x = pltpu.make_async_copy(ens, xin, load_sem.at[0])
    load_t = pltpu.make_async_copy(tru, tin, load_sem.at[1])
    load_w = pltpu.make_async_copy(w_hbm, w_ref, load_sem.at[2])
    load_w.start()
    load_x.start()
    load_t.start()

    @pl.when(odd)
    def _():
        pl.semaphore_wait(barrier, GROUPS - 1)
        pl.semaphore_signal(ready, inc=1, device_id=column(3), device_id_type=MESH)

    @pl.when(even)
    def _():
        pl.semaphore_wait(ready, 1)


    n = len(CHUNKS)

    def remote(src, dst, send, recv, d):
        return pltpu.make_async_remote_copy(
            src_ref=src, dst_ref=dst, send_sem=send, recv_sem=recv,
            device_id=column(d), device_id_type=MESH,
        )

    def values_copy(c, d, owner=None):
        to = lax.rem(me + d, GROUPS)
        if c == n:
            src = ex.at[:, pl.ds(FIRST[owner], DEAL[owner])]
            dst = rex.at[d - 1, :, pl.ds(0, DEAL[owner])]
        else:
            at, wide = CHUNKS[c]
            src = xin.at[:, pl.ds(2 * to, 2), :, pl.ds(at, wide)]
            dst = rv.at[d - 1, :, :, :, pl.ds(at, wide)]
        return remote(src, dst, send_v.at[c, d - 1], recv_v.at[c, d - 1], d)

    def grads_copy(c, d, owner=None):
        if c == n:
            src = gex.at[d - 1, :, pl.ds(0, DEAL[owner])]
            dst = oex.at[:, pl.ds(FIRST[owner], DEAL[owner])]
        else:
            at, wide = CHUNKS[c]
            src = gv.at[d - 1, :, :, :, pl.ds(at, wide)]
            dst = out.at[:, pl.ds(2 * me, 2), :, pl.ds(at, wide)]
        return remote(src, dst, send_g.at[c, d - 1], recv_g.at[c, d - 1], GROUPS - d)

    def one(make, c, d, act, owner):
        if c < n:
            act(make(c, d))
            return
        for rank in range(GROUPS):

            @pl.when(owner == rank)
            def _():
                act(make(c, d, rank))

    def each(make, c, act, to_peer):
        for d in hops:
            one(make, c, d, act, lax.rem(me + d, GROUPS) if to_peer else me)

    order = (0, n) + tuple(range(1, n))

    def send_back(pieces):
        for c, d in pieces:
            one(grads_copy, c, d, lambda copy: copy.start(), me)

    hops = (2, 1, 3)
    start = lambda copy: copy.start()
    landed = lambda copy: copy.wait_recv()
    left = lambda copy: copy.wait_send()
    load_x.wait()
    each(values_copy, 0, start, True)
    load_t.wait()
    load_w.wait()

    def pack(src, dst):
        for k in range(FULL // LANE):
            dst[k] = src[rows - 1, :, k * LANE : (k + 1) * LANE]
        wide = src.shape[-1] - FULL
        per = LANE // wide
        for g in range(EXTRA - FULL // LANE):
            parts = [
                src[r, :, FULL:].astype(jnp.float32)
                if r < rows
                else jnp.zeros((SUB, wide), jnp.float32)
                for r in range(g * per, (g + 1) * per)
            ]
            dst[FULL // LANE + g] = jnp.concatenate(parts, axis=1).astype(jnp.bfloat16)

    pack(tin, tex)

    @pl.loop(0, local)
    def _(m):
        pack(xin.at[m], ex.at[m])

    for c in order[1:]:
        each(values_copy, c, start, True)

    weight = w_ref[0]
    cells[...] = jnp.zeros_like(cells)

    def chunk_tiles(c):
        if c == n:
            first, many = FIRST[0], DEAL[0]
            for rank in range(1, GROUPS):
                first = jnp.where(me == rank, FIRST[rank], first)
                many = jnp.where(me == rank, DEAL[rank], many)

            def body(k, carry):
                mine = ex[:, first + k]
                x = jnp.concatenate([mine] + [rex[d, :, k] for d in range(GROUPS - 1)], axis=0)
                cell, grad = tile_terms(
                    x.astype(jnp.float32), tex[first + k].astype(jnp.float32), weight, members - 1
                )
                cells[...] += cell
                oex[:, first + k] = grad[:local]
                for d in range(GROUPS - 1):
                    gex[d, :, k] = grad[(d + 1) * local : (d + 2) * local]
                return carry

            lax.fori_loop(0, many, body, 0)
        else:
            at, wide = CHUNKS[c]
            tiles = wide // LANE

            def body(k, carry):
                r = k // tiles
                lanes = pl.ds(pl.multiple_of(at + (k - r * tiles) * LANE, LANE), LANE)
                mine = xin[:, 2 * me + r, :, lanes]
                x = jnp.concatenate(
                    [mine] + [rv[d, :, r, :, lanes] for d in range(GROUPS - 1)], axis=0
                )
                cell, grad = tile_terms(
                    x.astype(jnp.float32),
                    tin[2 * me + r, :, lanes].astype(jnp.float32),
                    weight,
                    members - 1,
                )
                cells[...] += cell
                out[:, 2 * me + r, :, lanes] = grad[:local]
                for d in range(GROUPS - 1):
                    gv[d, :, r, :, lanes] = grad[(d + 1) * local : (d + 2) * local]
                return carry

            lax.fori_loop(0, 2 * tiles, body, 0)

    for c in order:
        each(values_copy, c, landed, False)
        chunk_tiles(c)

        @pl.when(even)
        def _():
            if c != order[-1]:
                send_back([(c, d) for d in (2, 1, 3)])

        @pl.when(odd)
        def _():
            send_back([(c, d) for d in ((3, 1, 2) if c == 0 else (1, 2))])

    part[...] = jnp.sum(cells[...], axis=0, keepdims=True) * (weight * scale)
    hand = pltpu.make_async_remote_copy(
        src_ref=part, dst_ref=gift, send_sem=send_t.at[0], recv_sem=recv_t.at[0],
        device_id=column(1), device_id_type=MESH,
    )

    def tell(half, d):
        return pltpu.make_async_remote_copy(
            src_ref=part, dst_ref=totals.at[half], send_sem=send_t.at[d],
            recv_sem=recv_t.at[1 + half], device_id=column(d), device_id_type=MESH,
        )

    half = me // 2

    @pl.when(odd)
    def _():
        hand.start()
        send_back([(c, 3) for c in order[1:]])

    @pl.when(even)
    def _():
        pl.semaphore_wait(barrier, plane - 1)
        hand.wait_recv()
        part[...] += gift[...]

        def share(k):
            return pltpu.make_async_remote_copy(
                src_ref=part, dst_ref=stage.at[lat], send_sem=send_s.at[k - 1],
                recv_sem=recv_s.at[k - 1], device_id={"lat": lax.rem(lat + k, plane)},
                device_id_type=MESH,
            )

        @pl.loop(1, plane)
        def _(k):
            share(k).start()

        stage[lat] = part[...]

        @pl.loop(1, plane)
        def _(k):
            share(k).wait()

        part[...] = jnp.sum(stage[...], axis=0)
        for d in hops:
            tell(half, d).start()
        totals[half] = part[...]
        send_back([(order[-1], d) for d in hops])

    each(grads_copy, n, landed, True)

    @pl.loop(0, local)
    def _(m):
        for k in range(FULL // LANE):
            out[m, rows - 1, :, k * LANE : (k + 1) * LANE] = oex[m, k]
        wide = out.shape[-1] - FULL
        per = LANE // wide
        for g in range(-(-rows // per)):
            tile = oex[m, FULL // LANE + g].astype(jnp.float32)
            for j in range(per):
                if g * per + j < rows:
                    out[m, g * per + j, :, FULL:] = tile[:, j * wide : (j + 1) * wide].astype(
                        jnp.bfloat16
                    )

    @pl.when(even)
    def _():
        tell(1 - half, 2).wait_recv()
        for d in hops:
            tell(half, d).wait_send()

    @pl.when(odd)
    def _():
        for k in range(2):
            tell(k, 1).wait_recv()
        hand.wait_send()

    loss[...] = jnp.full(loss.shape, jnp.sum(totals[0] + totals[1]))

    for c in range(n):
        each(grads_copy, c, landed, True)
    for c in order:
        each(values_copy, c, left, True)
        each(grads_copy, c, left, False)


def hand_over(loss, grads, loss_out, grads_out, loss_at, sems):
    copies = [
        pltpu.make_async_copy(grads.at[m], grads_out.at[m], sems.at[m])
        for m in range(grads.shape[0])
    ]
    for copy in copies:
        copy.start()
    loss_at[0] = loss[0, 0]
    last = pltpu.make_async_copy(loss_at, loss_out, sems.at[grads.shape[0]])
    last.start()
    for copy in copies:
        copy.wait()
    last.wait()


def on_device(total_cells, ensemble, truth, row_weight):
    local, channels, _, lon = ensemble.shape
    rows = channels // SUB
    peers = GROUPS - 1
    plane = lax.axis_size("lat")
    n_copies = len(CHUNKS) + 1
    bf = jnp.bfloat16
    loss, out = pl.pallas_call(
        functools.partial(
            lambda l, s, e, t, w, o, z, *rest: kernel(l, s, e, t, w, z, o, *rest),
            plane,
            1.0 / (local * GROUPS) / total_cells,
        ),
        out_shape=(
            jax.ShapeDtypeStruct((1, LANE), jnp.float32),
            jax.ShapeDtypeStruct((local, rows, SUB, lon), bf),
        ),
        in_specs=[
            pl.BlockSpec(memory_space=pl.ANY),
            pl.BlockSpec(memory_space=pl.ANY),
            pl.BlockSpec(memory_space=pltpu.HBM),
        ],
        out_specs=(
            pl.BlockSpec(memory_space=pltpu.VMEM),
            pl.BlockSpec(memory_space=pltpu.VMEM),
        ),
        scratch_shapes=[
            pltpu.VMEM((local, rows, SUB, lon), bf),
            pltpu.VMEM((rows, SUB, lon), bf),
            pltpu.VMEM((local, EXTRA, SUB, LANE), bf),
            pltpu.VMEM((EXTRA, SUB, LANE), bf),
            pltpu.VMEM((peers, local, 2, SUB, FULL), bf),
            pltpu.VMEM((peers, local, max(DEAL), SUB, LANE), bf),
            pltpu.VMEM((peers, local, 2, SUB, FULL), bf),
            pltpu.VMEM((peers, local, max(DEAL), SUB, LANE), bf),
            pltpu.VMEM((local, EXTRA, SUB, LANE), bf),
            pltpu.VMEM((SUB, LANE), jnp.float32),
            pltpu.VMEM((1, LANE), jnp.float32),
            pltpu.VMEM((1, LANE), jnp.float32),
            pltpu.VMEM((plane, 1, LANE), jnp.float32),
            pltpu.VMEM((2, 1, LANE), jnp.float32),
            pltpu.SMEM((1,), jnp.float32),
            pltpu.SemaphoreType.DMA((3,)),
            pltpu.SemaphoreType.DMA((n_copies, peers)),
            pltpu.SemaphoreType.DMA((n_copies, peers)),
            pltpu.SemaphoreType.DMA((n_copies, peers)),
            pltpu.SemaphoreType.DMA((n_copies, peers)),
            pltpu.SemaphoreType.DMA((plane - 1,)),
            pltpu.SemaphoreType.DMA((plane - 1,)),
            pltpu.SemaphoreType.DMA((GROUPS,)),
            pltpu.SemaphoreType.DMA((3,)),
            pltpu.SemaphoreType.REGULAR,
        ],
        compiler_params=pltpu.CompilerParams(
            collective_id=0, has_side_effects=True, vmem_limit_bytes=48 * 1024 * 1024
        ),
        name="crps_exchange",
    )(
        pltpu.with_memory_space_constraint(ensemble.reshape(local, rows, SUB, lon), pltpu.HBM),
        pltpu.with_memory_space_constraint(truth.reshape(rows, SUB, lon), pltpu.HBM),
        row_weight,
    )
    loss, out = pl.pallas_call(
        hand_over,
        out_shape=(
            jax.ShapeDtypeStruct((1,), jnp.float32),
            jax.ShapeDtypeStruct(out.shape, out.dtype),
        ),
        in_specs=[pl.BlockSpec(memory_space=pltpu.VMEM)] * 2,
        out_specs=(pl.BlockSpec(memory_space=pl.ANY), pl.BlockSpec(memory_space=pl.ANY)),
        scratch_shapes=[pltpu.SMEM((1,), jnp.float32), pltpu.SemaphoreType.DMA((local + 1,))],
        compiler_params=pltpu.CompilerParams(vmem_limit_bytes=4 * 1024 * 1024),
        name="hand_over",
    )(loss, out)
    return loss.reshape(()), out.reshape(ensemble.shape)


def solution(mesh):
    def whole(ensemble, truth, row_weight):
        cells = truth.size
        step = jax.shard_map(
            functools.partial(on_device, cells),
            mesh=mesh,
            in_specs=(P("mem", None, "lat", None), P(None, "lat", None), P("lat")),
            out_specs=(P(), P("mem", None, "lat", None)),
            check_vma=False,
        )
        return step(ensemble, truth, row_weight)

    return whole
```

```python
import functools

import jax
import jax.numpy as jnp
from jax import lax
from jax.experimental import pallas as pl
from jax.experimental.pallas import tpu as pltpu
from jax.sharding import PartitionSpec as P

MESH = pl.DeviceIdType.MESH
GROUPS = 4
SUB = 8
LANE = 128
CHUNKS = ((0, 512), (512, 384), (896, 384), (1280, 128))
FULL = 1408
DEAL = (3, 4, 3, 4)
EXTRA = sum(DEAL)
FIRST = tuple(sum(DEAL[:rank]) for rank in range(GROUPS))


def spread_out(x):
    tiny = jnp.minimum(jnp.maximum(x, -(2.0**-113)), 2.0**-113)
    return tiny * 2.0**66 * 2.0**67 + x * 2.0**124


def sign_of(left, right):
    return jnp.minimum(jnp.maximum(left - right, -1.0), 1.0)


def counts_of(x):
    members = x.shape[0]
    count = jnp.zeros_like(x)
    for step in range(1, members // 2 + 1):
        if 2 * step == members:
            s = sign_of(x[:step], x[step:])
            count = count + jnp.concatenate([s, -s], axis=0)
        else:
            s = sign_of(x, jnp.concatenate([x[step:], x[:step]], axis=0))
            count = count + (s - jnp.concatenate([s[-step:], s[:-step]], axis=0))
    return count


def tile_terms(x, t, weight, pairs):
    place = spread_out(x)
    count = counts_of(place) * (1.0 / pairs)
    skill = jnp.abs(x - t[None])
    cell = jnp.sum(skill - x * count, axis=0)
    grad = weight * (sign_of(place, spread_out(t)[None]) - count)
    return cell, grad.astype(jnp.bfloat16)


def kernel(
    plane, scale, ens, tru, w_hbm, out, loss, xin, tin, ex, tex, rv, rex, gv, gex, oex,
    cells, part, gift, stage, totals, w_ref, load_sem, send_v, recv_v, send_g, recv_g, send_s, recv_s,
    send_t, recv_t, ready,
):
    me = lax.axis_index("mem")
    lat = lax.axis_index("lat")
    local = ens.shape[0]
    members = local * GROUPS
    rows = ens.shape[1]

    def column(d):
        return {"mem": lax.rem(me + d, GROUPS)}

    even = lax.rem(me, 2) == 0
    odd = lax.rem(me, 2) == 1

    barrier = pltpu.get_barrier_semaphore()

    def greet(where):
        pl.semaphore_signal(barrier, inc=1, device_id=where, device_id_type=MESH)

    @pl.when(odd)
    def _():
        greet(column(2))

    @pl.when(even)
    def _():
        for d in (1, 3):
            greet(column(d))

        @pl.loop(1, plane)
        def _(k):
            greet({"lat": lax.rem(lat + k, plane)})

    load_x = pltpu.make_async_copy(ens, xin, load_sem.at[0])
    load_t = pltpu.make_async_copy(tru, tin, load_sem.at[1])
    load_w = pltpu.make_async_copy(w_hbm, w_ref, load_sem.at[2])
    load_w.start()
    load_x.start()
    load_t.start()

    @pl.when(odd)
    def _():
        pl.semaphore_wait(barrier, GROUPS - 1)
        pl.semaphore_signal(ready, inc=1, device_id=column(3), device_id_type=MESH)

    @pl.when(even)
    def _():
        pl.semaphore_wait(ready, 1)


    n = len(CHUNKS)

    def remote(src, dst, send, recv, d):
        return pltpu.make_async_remote_copy(
            src_ref=src, dst_ref=dst, send_sem=send, recv_sem=recv,
            device_id=column(d), device_id_type=MESH,
        )

    def values_copy(c, d, owner=None):
        to = lax.rem(me + d, GROUPS)
        if c == n:
            src = ex.at[:, pl.ds(FIRST[owner], DEAL[owner])]
            dst = rex.at[d - 1, :, pl.ds(0, DEAL[owner])]
        else:
            at, wide = CHUNKS[c]
            src = xin.at[:, pl.ds(2 * to, 2), :, pl.ds(at, wide)]
            dst = rv.at[d - 1, :, :, :, pl.ds(at, wide)]
        return remote(src, dst, send_v.at[c, d - 1], recv_v.at[c, d - 1], d)

    def grads_copy(c, d, owner=None):
        if c == n:
            src = gex.at[d - 1, :, pl.ds(0, DEAL[owner])]
            dst = oex.at[:, pl.ds(FIRST[owner], DEAL[owner])]
        else:
            at, wide = CHUNKS[c]
            src = gv.at[d - 1, :, :, :, pl.ds(at, wide)]
            dst = out.at[:, pl.ds(2 * me, 2), :, pl.ds(at, wide)]
        return remote(src, dst, send_g.at[c, d - 1], recv_g.at[c, d - 1], GROUPS - d)

    def one(make, c, d, act, owner):
        if c < n:
            act(make(c, d))
            return
        for rank in range(GROUPS):

            @pl.when(owner == rank)
            def _():
                act(make(c, d, rank))

    def each(make, c, act, to_peer):
        for d in hops:
            one(make, c, d, act, lax.rem(me + d, GROUPS) if to_peer else me)

    order = (0, n) + tuple(range(1, n))

    def send_back(pieces):
        for c, d in pieces:
            one(grads_copy, c, d, lambda copy: copy.start(), me)

    hops = (2, 3, 1)
    start = lambda copy: copy.start()
    landed = lambda copy: copy.wait_recv()
    left = lambda copy: copy.wait_send()
    load_x.wait()
    each(values_copy, 0, start, True)
    load_t.wait()
    load_w.wait()

    def pack(src, dst):
        for k in range(FULL // LANE):
            dst[k] = src[rows - 1, :, k * LANE : (k + 1) * LANE]
        wide = src.shape[-1] - FULL
        per = LANE // wide
        for g in range(EXTRA - FULL // LANE):
            parts = [
                src[r, :, FULL:].astype(jnp.float32)
                if r < rows
                else jnp.zeros((SUB, wide), jnp.float32)
                for r in range(g * per, (g + 1) * per)
            ]
            dst[FULL // LANE + g] = jnp.concatenate(parts, axis=1).astype(jnp.bfloat16)

    pack(tin, tex)

    @pl.loop(0, local)
    def _(m):
        pack(xin.at[m], ex.at[m])

    for c in order[1:]:
        each(values_copy, c, start, True)

    weight = w_ref[0]
    cells[...] = jnp.zeros_like(cells)

    def chunk_tiles(c):
        if c == n:
            first, many = FIRST[0], DEAL[0]
            for rank in range(1, GROUPS):
                first = jnp.where(me == rank, FIRST[rank], first)
                many = jnp.where(me == rank, DEAL[rank], many)

            def body(k, carry):
                mine = ex[:, first + k]
                x = jnp.concatenate([mine] + [rex[d, :, k] for d in range(GROUPS - 1)], axis=0)
                cell, grad = tile_terms(
                    x.astype(jnp.float32), tex[first + k].astype(jnp.float32), weight, members - 1
                )
                cells[...] += cell
                oex[:, first + k] = grad[:local]
                for d in range(GROUPS - 1):
                    gex[d, :, k] = grad[(d + 1) * local : (d + 2) * local]
                return carry

            lax.fori_loop(0, many, body, 0)
        else:
            at, wide = CHUNKS[c]
            tiles = wide // LANE

            def body(k, carry):
                r = k // tiles
                lanes = pl.ds(pl.multiple_of(at + (k - r * tiles) * LANE, LANE), LANE)
                mine = xin[:, 2 * me + r, :, lanes]
                x = jnp.concatenate(
                    [mine] + [rv[d, :, r, :, lanes] for d in range(GROUPS - 1)], axis=0
                )
                cell, grad = tile_terms(
                    x.astype(jnp.float32),
                    tin[2 * me + r, :, lanes].astype(jnp.float32),
                    weight,
                    members - 1,
                )
                cells[...] += cell
                out[:, 2 * me + r, :, lanes] = grad[:local]
                for d in range(GROUPS - 1):
                    gv[d, :, r, :, lanes] = grad[(d + 1) * local : (d + 2) * local]
                return carry

            lax.fori_loop(0, 2 * tiles, body, 0)

    for c in order:
        each(values_copy, c, landed, False)
        chunk_tiles(c)

        @pl.when(even)
        def _():
            if c != order[-1]:
                send_back([(c, d) for d in (2, 1, 3)])

        @pl.when(odd)
        def _():
            send_back([(c, d) for d in ((3, 1, 2) if c == 0 else (1, 2))])

    part[...] = jnp.sum(cells[...], axis=0, keepdims=True) * (weight * scale)
    hand = pltpu.make_async_remote_copy(
        src_ref=part, dst_ref=gift, send_sem=send_t.at[0], recv_sem=recv_t.at[0],
        device_id=column(1), device_id_type=MESH,
    )

    def tell(half, d):
        return pltpu.make_async_remote_copy(
            src_ref=part, dst_ref=totals.at[half], send_sem=send_t.at[d],
            recv_sem=recv_t.at[1 + half], device_id=column(d), device_id_type=MESH,
        )

    half = me // 2

    @pl.when(odd)
    def _():
        hand.start()
        send_back([(c, 3) for c in order[1:]])

    @pl.when(even)
    def _():
        pl.semaphore_wait(barrier, plane - 1)
        hand.wait_recv()
        part[...] += gift[...]

        def share(k):
            return pltpu.make_async_remote_copy(
                src_ref=part, dst_ref=stage.at[lat], send_sem=send_s.at[k - 1],
                recv_sem=recv_s.at[k - 1], device_id={"lat": lax.rem(lat + k, plane)},
                device_id_type=MESH,
            )

        @pl.loop(1, plane)
        def _(k):
            share(k).start()

        stage[lat] = part[...]

        @pl.loop(1, plane)
        def _(k):
            share(k).wait()

        part[...] = jnp.sum(stage[...], axis=0)
        for d in hops:
            tell(half, d).start()
        totals[half] = part[...]
        send_back([(order[-1], d) for d in hops])

    each(grads_copy, n, landed, True)

    @pl.loop(0, local)
    def _(m):
        for k in range(FULL // LANE):
            out[m, rows - 1, :, k * LANE : (k + 1) * LANE] = oex[m, k]
        wide = out.shape[-1] - FULL
        per = LANE // wide
        for g in range(-(-rows // per)):
            tile = oex[m, FULL // LANE + g].astype(jnp.float32)
            for j in range(per):
                if g * per + j < rows:
                    out[m, g * per + j, :, FULL:] = tile[:, j * wide : (j + 1) * wide].astype(
                        jnp.bfloat16
                    )

    @pl.when(even)
    def _():
        tell(1 - half, 2).wait_recv()
        for d in hops:
            tell(half, d).wait_send()

    @pl.when(odd)
    def _():
        for k in range(2):
            tell(k, 1).wait_recv()
        hand.wait_send()

    loss[...] = jnp.full(loss.shape, jnp.sum(totals[0] + totals[1]))

    for c in range(n):
        each(grads_copy, c, landed, True)
    for c in order:
        each(values_copy, c, left, True)
        each(grads_copy, c, left, False)


def hand_over(loss, grads, loss_out, grads_out, loss_at, sems):
    copies = [
        pltpu.make_async_copy(grads.at[m], grads_out.at[m], sems.at[m])
        for m in range(grads.shape[0])
    ]
    for copy in copies:
        copy.start()
    loss_at[0] = loss[0, 0]
    last = pltpu.make_async_copy(loss_at, loss_out, sems.at[grads.shape[0]])
    last.start()
    for copy in copies:
        copy.wait()
    last.wait()


def on_device(total_cells, ensemble, truth, row_weight):
    local, channels, _, lon = ensemble.shape
    rows = channels // SUB
    peers = GROUPS - 1
    plane = lax.axis_size("lat")
    n_copies = len(CHUNKS) + 1
    bf = jnp.bfloat16
    loss, out = pl.pallas_call(
        functools.partial(
            lambda l, s, e, t, w, o, z, *rest: kernel(l, s, e, t, w, z, o, *rest),
            plane,
            1.0 / (local * GROUPS) / total_cells,
        ),
        out_shape=(
            jax.ShapeDtypeStruct((1, LANE), jnp.float32),
            jax.ShapeDtypeStruct((local, rows, SUB, lon), bf),
        ),
        in_specs=[
            pl.BlockSpec(memory_space=pl.ANY),
            pl.BlockSpec(memory_space=pl.ANY),
            pl.BlockSpec(memory_space=pltpu.HBM),
        ],
        out_specs=(
            pl.BlockSpec(memory_space=pltpu.VMEM),
            pl.BlockSpec(memory_space=pltpu.VMEM),
        ),
        scratch_shapes=[
            pltpu.VMEM((local, rows, SUB, lon), bf),
            pltpu.VMEM((rows, SUB, lon), bf),
            pltpu.VMEM((local, EXTRA, SUB, LANE), bf),
            pltpu.VMEM((EXTRA, SUB, LANE), bf),
            pltpu.VMEM((peers, local, 2, SUB, FULL), bf),
            pltpu.VMEM((peers, local, max(DEAL), SUB, LANE), bf),
            pltpu.VMEM((peers, local, 2, SUB, FULL), bf),
            pltpu.VMEM((peers, local, max(DEAL), SUB, LANE), bf),
            pltpu.VMEM((local, EXTRA, SUB, LANE), bf),
            pltpu.VMEM((SUB, LANE), jnp.float32),
            pltpu.VMEM((1, LANE), jnp.float32),
            pltpu.VMEM((1, LANE), jnp.float32),
            pltpu.VMEM((plane, 1, LANE), jnp.float32),
            pltpu.VMEM((2, 1, LANE), jnp.float32),
            pltpu.SMEM((1,), jnp.float32),
            pltpu.SemaphoreType.DMA((3,)),
            pltpu.SemaphoreType.DMA((n_copies, peers)),
            pltpu.SemaphoreType.DMA((n_copies, peers)),
            pltpu.SemaphoreType.DMA((n_copies, peers)),
            pltpu.SemaphoreType.DMA((n_copies, peers)),
            pltpu.SemaphoreType.DMA((plane - 1,)),
            pltpu.SemaphoreType.DMA((plane - 1,)),
            pltpu.SemaphoreType.DMA((GROUPS,)),
            pltpu.SemaphoreType.DMA((3,)),
            pltpu.SemaphoreType.REGULAR,
        ],
        compiler_params=pltpu.CompilerParams(
            collective_id=0, has_side_effects=True, vmem_limit_bytes=48 * 1024 * 1024
        ),
        name="crps_exchange",
    )(
        pltpu.with_memory_space_constraint(ensemble.reshape(local, rows, SUB, lon), pltpu.HBM),
        pltpu.with_memory_space_constraint(truth.reshape(rows, SUB, lon), pltpu.HBM),
        row_weight,
    )
    loss, out = pl.pallas_call(
        hand_over,
        out_shape=(
            jax.ShapeDtypeStruct((1,), jnp.float32),
            jax.ShapeDtypeStruct(out.shape, out.dtype),
        ),
        in_specs=[pl.BlockSpec(memory_space=pltpu.VMEM)] * 2,
        out_specs=(pl.BlockSpec(memory_space=pl.ANY), pl.BlockSpec(memory_space=pl.ANY)),
        scratch_shapes=[pltpu.SMEM((1,), jnp.float32), pltpu.SemaphoreType.DMA((local + 1,))],
        compiler_params=pltpu.CompilerParams(vmem_limit_bytes=4 * 1024 * 1024),
        name="hand_over",
    )(loss, out)
    return loss.reshape(()), out.reshape(ensemble.shape)


def solution(mesh):
    def whole(ensemble, truth, row_weight):
        cells = truth.size
        step = jax.shard_map(
            functools.partial(on_device, cells),
            mesh=mesh,
            in_specs=(P("mem", None, "lat", None), P(None, "lat", None), P("lat")),
            out_specs=(P(), P("mem", None, "lat", None)),
            check_vma=False,
        )
        return step(ensemble, truth, row_weight)

    return whole
```
